128 devices in a mesh: lat: 16 (over x, z), lon: 8 (over y, core).
Axes of the slice: x: 4, y: 4, z: 4, core: 2. Of those that a mesh axis runs over, the one named last changes fastest.
Arguments:
- increment: bfloat16 [32, 16, 144, 128], P('lat', 'lon'), may hold values from -6 to 6
- cotangent: bfloat16 [16, 8, 40, 144, 128], P('lat', 'lon'), may hold values from -6 to 6
- weights: bfloat16 [16, 8, 40, 16, 128, 128], P('lat', 'lon'), may hold values from -0.1875 to 0.1875
- source_ids: int32 [16, 8, 40, 16], P('lat', 'lon'), may hold values from 0 to 511, as said below
- counts: int32 [16, 8, 40], P('lat', 'lon'), may hold values from 0 to 16, as said below
Outputs:
- ocean: bfloat16 [16, 8, 40, 144, 128], P('lat', 'lon')
- atmos_adjoint: bfloat16 [32, 16, 144, 128], P('lat', 'lon')
The draws below stay inside these ranges and needn't reach their ends.
Inputs may be any that keep to these rules, and one draw needn't show every extreme that they name: source_ids[i, j, t, k] = a * 16 + b with block row a between i * 2 - 1 and (i + 1) * 2, and block column b equal, modulo 16, to one of j * 2 - 1 to (j + 1) * 2. `counts`: every device's tile (i, j) has some target block with exactly 16 live slots.
All inputs are finite; a program needn't handle non-finite values.
Results may differ from the reference program's by a relative error of at most 0.001.
Values may be sent and summed in bfloat16 or wider, within the bound.
A program may use at most 192 MiB of HBM per device.

```python
import jax
import jax.numpy as jnp
from jax import lax

BS = 128
BT = 128
SBD = 2
TB = 40
KPT = 16
ROWS = 144
NLB = 32
NOB = 16
N_LAT = 16
N_LON = 8


def draw_source_ids(key, part):
    key_rows, key_cols = jax.random.split(jax.random.fold_in(key, 11))
    shape = (N_LAT, N_LON, TB, KPT)
    lat_grid = jnp.arange(N_LAT, dtype=jnp.int32)[:, None, None, None]
    lon_grid = jnp.arange(N_LON, dtype=jnp.int32)[None, :, None, None]
    lowest = jnp.where(lat_grid == 0, 1, 0)
    highest = jnp.where(lat_grid == N_LAT - 1, SBD, SBD + 1)
    raw_rows = jax.random.randint(key_rows, shape, 0, 1 << 20)
    ext_row = lowest + raw_rows % (highest - lowest + 1)
    ext_col = jax.random.randint(key_cols, shape, 0, SBD + 2)
    cycle_blocks = SBD * N_LON
    block_row = lat_grid * SBD + ext_row - 1
    block_col = (lon_grid * SBD + ext_col - 1 + cycle_blocks) % cycle_blocks
    return (block_row * cycle_blocks + block_col).astype(jnp.int32)


def draw_counts(key, part):
    key_rows, key_cols = jax.random.split(jax.random.fold_in(key, 23))
    drawn = jax.random.randint(key_rows, (N_LAT, N_LON, TB), 0, KPT + 1)
    full_slot = jax.random.randint(key_cols, (N_LAT, N_LON, 1), 0, TB)
    target_index = jnp.arange(TB, dtype=jnp.int32)[None, None, :]
    return jnp.where(target_index == full_slot, KPT, drawn).astype(jnp.int32)


def block_levels(key, extent, cuts, low, largest):
    factor_of = 1.0
    for dim, blocks in cuts:
        steps = jax.random.uniform(jax.random.fold_in(jax.random.fold_in(key, 6), dim), (blocks,), jnp.float32, low / len(cuts), largest / len(cuts))
        factor_of = factor_of * jnp.repeat(jnp.exp(steps), extent[dim] // blocks).reshape((-1,) + (1,) * (len(extent) - 1 - dim))
    return factor_of


def scatter_about(key, extent, width, limit, cuts=(), kind=jnp.bfloat16):
    gain = block_levels(key, extent, cuts, -0.22, 0.18) if cuts else 1.0
    entries = jax.random.normal(key, extent, jnp.float32) * width * gain
    return jnp.minimum(jnp.maximum(entries, -limit), limit).astype(kind)


def setup_inputs(seed: int = 0) -> dict:
    streams_of = jax.random.split(jax.random.key(seed), 6)
    return {
        "increment": scatter_about(streams_of[0], (NLB, NOB, ROWS, BS), 1.0, 6.0, ((0, 16), (1, 8))),
        "cotangent": scatter_about(streams_of[1], (N_LAT, N_LON, TB, ROWS, BT), 1.0, 6.0, ((0, 16), (1, 8))),
        "weights": scatter_about(streams_of[2], (N_LAT, N_LON, TB, KPT, BS, BT), (BS * KPT // 2) ** -0.5, 0.1875, ((0, 16), (1, 8))),
        "source_ids": draw_source_ids(jax.random.fold_in(streams_of[5], 71), 0),
        "counts": draw_counts(jax.random.fold_in(streams_of[5], 71), 0),
    }


def reference(increment, cotangent, weights, source_ids, counts):
    total_blocks = NLB * NOB
    device_count = N_LAT * N_LON
    flattened = increment.reshape(total_blocks, ROWS, BS)
    weight_all = weights.reshape(device_count, TB, KPT, BS, BT)
    source_all = source_ids.reshape(device_count, TB, KPT).astype(jnp.int32)
    count_all = counts.reshape(device_count, TB).astype(jnp.int32)
    cotan_all = cotangent.reshape(device_count, TB, ROWS, BT)

    def device_step(running, pieces):
        weight_dev, source_dev, count_dev, cotan_dev = pieces
        ocean_sum = jnp.zeros((TB, ROWS, BT), jnp.float32)
        cotan_wide = cotan_dev.astype(jnp.float32)
        for slot in range(KPT):
            active = slot < count_dev
            weight_slot = weight_dev[:, slot].astype(jnp.float32)
            picked = flattened[source_dev[:, slot]].astype(jnp.float32) * active.astype(jnp.float32)[:, None, None]
            ocean_sum = ocean_sum + jnp.einsum("tws,tsb->twb", picked, weight_slot)
            contribution = jnp.einsum("twb,tsb->tws", cotan_wide, weight_slot)
            segment = jnp.where(active, source_dev[:, slot], total_blocks).astype(jnp.int32)
            running = running.at[segment].add(contribution)
        return running, ocean_sum.astype(jnp.bfloat16)

    running = jnp.zeros((total_blocks + 1, ROWS, BS), jnp.float32)
    running, ocean = lax.scan(device_step, running, (weight_all, source_all, count_all, cotan_all))
    ocean = ocean.reshape(N_LAT, N_LON, TB, ROWS, BT)
    adjoint_out = running[:total_blocks].reshape(NLB, NOB, ROWS, BS).astype(jnp.bfloat16)
    return ocean, adjoint_out
```

```python
import functools

import jax
import jax.numpy as jnp
from jax import lax
from jax.experimental import pallas as pl
from jax.experimental.pallas import tpu as pltpu
from jax.sharding import PartitionSpec as P

MESH = pl.DeviceIdType.MESH
CHAINS = 4
GROUP = 4
RING = 4

HALO = [(r, c) for r in range(4) for c in range(4) if r in (0, 3) or c in (0, 3)]
STEP = {0: -1, 1: 0, 2: 0, 3: 1}
SEND_ORDER = sorted(range(len(HALO)), key=lambda h: STEP[HALO[h][0]] == 0)


def kernel(
    lat_count, lon_count, targets, slots,
    table, inc_hbm, cot_hbm, w_hbm, ocean_hbm, adj_hbm,
    wbuf, cot, ext, d0, d1, d2, d3, obuf, sendb, recvb, abuf,
    w_sem, cot_sem, own_sem, inc_send, inc_recv, adj_send, adj_recv, out_sem, adj_sem,
):
    lat = lax.axis_index("lat")
    lon = lax.axis_index("lon")
    chains = (d0, d1, d2, d3)
    groups = targets // GROUP
    quads = slots // CHAINS
    entries = targets * quads
    rows, cells = ext.shape[1], ext.shape[2]
    total = targets * slots

    def load_w(g, slot, tt):
        return pltpu.make_async_copy(
            w_hbm.at[0, 0, g * GROUP + tt], wbuf.at[slot, tt], w_sem.at[slot, tt]
        )

    def load_cot(g):
        return pltpu.make_async_copy(
            cot_hbm.at[0, 0, pl.ds(g * GROUP, GROUP)], cot.at[pl.ds(g * GROUP, GROUP)], cot_sem.at[g]
        )

    own = [
        pltpu.make_async_copy(inc_hbm.at[r], ext.at[pl.ds((r + 1) * 4 + 1, 2)], own_sem.at[r])
        for r in range(2)
    ]
    for copy in own:
        copy.start()
    for g in range(RING):
        load_cot(g).start()
        for tt in range(GROUP):
            load_w(g, g, tt).start()
    for g in range(RING, groups):
        load_cot(g).start()

    def exists(dlat):
        if dlat < 0:
            return lat > 0
        if dlat > 0:
            return lat < lat_count - 1
        return None

    def guarded(dlat, action):
        if dlat == 0:
            action()
        else:
            pl.when(exists(dlat))(action)

    def peer(dlat, dlon):
        return (lat + dlat, lax.rem(lon + dlon + lon_count, lon_count))

    barrier = pltpu.get_barrier_semaphore()
    around = [(a, b) for a in (-1, 0, 1) for b in (-1, 0, 1) if (a, b) != (0, 0)]
    for a, b in around:
        guarded(
            a,
            lambda a=a, b=b: pl.semaphore_signal(
                barrier, inc=1, device_id=peer(a, b), device_id_type=MESH
            ),
        )
    bands = exists(-1).astype(jnp.int32) + exists(1).astype(jnp.int32)
    pl.semaphore_wait(barrier, 2 + 3 * bands)

    zero = jnp.zeros((rows, cells), jnp.float32)
    ext[16] = zero.astype(ext.dtype)
    for d in chains:
        d[entries] = zero

    def inc_copy(h):
        r, c = HALO[h]
        dlat, dlon = -STEP[r], -STEP[c]
        src = (r - 1 + 2 * (-STEP[r])) + 1, (c - 1 + 2 * (-STEP[c])) + 1
        return dlat, pltpu.make_async_remote_copy(
            src_ref=ext.at[src[0] * 4 + src[1]],
            dst_ref=ext.at[r * 4 + c],
            send_sem=inc_send.at[h],
            recv_sem=inc_recv.at[h],
            device_id=peer(dlat, dlon),
            device_id_type=MESH,
        )

    def adj_copy(h):
        r, c = HALO[h]
        dlat, dlon = STEP[r], STEP[c]
        return dlat, pltpu.make_async_remote_copy(
            src_ref=sendb.at[h],
            dst_ref=recvb.at[h],
            send_sem=adj_send.at[h],
            recv_sem=adj_recv.at[h],
            device_id=peer(dlat, dlon),
            device_id_type=MESH,
        )

    for copy in own:
        copy.wait()
    for h in SEND_ORDER:
        dlat, copy = inc_copy(h)
        guarded(dlat, copy.start)

    def adjoint_group(g, carry):
        slot = lax.rem(g, RING)
        load_cot(g).wait()
        for tt in range(GROUP):
            load_w(g, slot, tt).wait()
        for tt in range(GROUP):
            t = g * GROUP + tt
            here = cot[t]
            for q in range(quads):
                w = wbuf[slot, tt, pl.ds(q * CHAINS, CHAINS)].reshape(CHAINS * cells, cells)
                product = lax.dot_general(
                    here, w, (((1,), (1,)), ((), ())), preferred_element_type=jnp.float32
                )
                for j in range(CHAINS):
                    before = table[total + t * slots + q * CHAINS + j]
                    chains[j][t * quads + q] = (
                        product[:, j * cells : (j + 1) * cells] + chains[j][before]
                    )

        @pl.when(g + RING < groups)
        def _():
            for tt in range(GROUP):
                load_w(g + RING, slot, tt).start()

        return carry

    lax.fori_loop(0, groups, adjoint_group, 0)

    def summed(position):
        parts = [chains[j][table[2 * total + position * CHAINS + j]] for j in range(CHAINS)]
        return (parts[0] + parts[1]) + (parts[2] + parts[3])

    for h in SEND_ORDER:
        r, c = HALO[h]
        sendb[h] = summed(r * 4 + c)
        dlat, copy = adj_copy(h)
        guarded(dlat, copy.start)

    for h in SEND_ORDER:
        dlat, copy = inc_copy(h)
        guarded(-dlat, copy.wait_recv)
        guarded(dlat, copy.wait_send)

    def ocean_copy(g):
        return pltpu.make_async_copy(
            obuf.at[pl.ds(g * GROUP, GROUP)], ocean_hbm.at[0, 0, pl.ds(g * GROUP, GROUP)], out_sem.at[g]
        )

    def forward_group(i, carry):
        g = groups - 1 - i
        slot = lax.rem(g, RING)

        @pl.when(g < groups - RING)
        def _():
            for tt in range(GROUP):
                load_w(g, slot, tt).wait()

        for tt in range(GROUP):
            t = g * GROUP + tt
            picked = jnp.concatenate([ext[table[t * slots + k]] for k in range(slots)], axis=1)
            w = wbuf[slot, tt].reshape(slots * cells, cells)
            obuf[t] = jnp.dot(picked, w, preferred_element_type=jnp.float32).astype(obuf.dtype)
        ocean_copy(g).start()

        @pl.when(g >= RING)
        def _():
            for tt in range(GROUP):
                load_w(g - RING, slot, tt).start()

        return carry

    lax.fori_loop(0, groups, forward_group, 0)

    index = {place: h for h, place in enumerate(HALO)}
    for dlat in (-1, 1):
        r = 0 if dlat < 0 else 3

        @pl.when(jnp.logical_not(exists(-dlat)))
        def _():
            for c in range(4):
                recvb[index[r, c]] = zero

    for h in SEND_ORDER:
        dlat, copy = adj_copy(h)
        guarded(-dlat, copy.wait_recv)
    for a in range(2):
        for b in range(2):
            far_r, far_c = (3 if a == 0 else 0), (3 if b == 0 else 0)
            value = summed((a + 1) * 4 + b + 1)
            value += recvb[index[far_r, b + 1]] + recvb[index[a + 1, far_c]]
            value += recvb[index[far_r, far_c]]
            abuf[a, b] = value.astype(abuf.dtype)
    final = pltpu.make_async_copy(abuf, adj_hbm, adj_sem)
    final.start()
    for h in SEND_ORDER:
        dlat, copy = adj_copy(h)
        guarded(dlat, copy.wait_send)
    for g in range(groups):
        ocean_copy(g).wait()
    final.wait()


def tables(source_ids, counts):
    ids = source_ids[0, 0]
    targets, slots = ids.shape
    quads = slots // CHAINS
    cycle = 2 * lax.axis_size("lon")
    row = ids // cycle - 2 * lax.axis_index("lat") + 1
    col = (ids % cycle - 2 * lax.axis_index("lon") + 1 + cycle) % cycle
    live = jnp.arange(slots, dtype=jnp.int32)[None, :] < counts[0, 0][:, None]
    position = jnp.where(live, row * 4 + col, 16)
    entries = targets * quads
    lanes = position.reshape(entries, CHAINS).T
    order = jnp.arange(entries, dtype=jnp.int32)
    same = (lanes[:, :, None] == lanes[:, None, :]) & (order[None, None, :] < order[None, :, None])
    before = jnp.max(jnp.where(same, order[None, None, :], -1), axis=2)
    before = jnp.where(before < 0, entries, before)
    places = jnp.arange(16, dtype=jnp.int32)
    final = jnp.max(
        jnp.where(lanes[:, None, :] == places[None, :, None], order[None, None, :], -1), axis=2
    )
    final = jnp.where(final < 0, entries, final)
    return jnp.concatenate(
        [position.reshape(-1), before.T.reshape(-1), final.T.reshape(-1)]
    )


def body(lat_count, lon_count, increment, cotangent, weights, source_ids, counts):
    targets, slots = weights.shape[2], weights.shape[3]
    rows, cells = increment.shape[2], increment.shape[3]
    table = tables(source_ids, counts)
    groups = targets // GROUP
    entries = targets * slots // CHAINS
    halo = len(HALO)
    any_space = pl.BlockSpec(memory_space=pl.ANY)
    dma = pltpu.SemaphoreType.DMA
    return pl.pallas_call(
        functools.partial(kernel, lat_count, lon_count, targets, slots),
        out_shape=(
            jax.ShapeDtypeStruct(cotangent.shape, jnp.bfloat16),
            jax.ShapeDtypeStruct(increment.shape, jnp.bfloat16),
        ),
        in_specs=[pl.BlockSpec(memory_space=pltpu.SMEM)] + [any_space] * 3,
        out_specs=(any_space, any_space),
        scratch_shapes=[
            pltpu.VMEM((RING, GROUP, slots, cells, cells), jnp.bfloat16),
            pltpu.VMEM((targets, rows, cells), jnp.bfloat16),
            pltpu.VMEM((17, rows, cells), jnp.bfloat16),
        ]
        + [pltpu.VMEM((entries + 1, rows, cells), jnp.float32)] * CHAINS
        + [
            pltpu.VMEM((targets, rows, cells), jnp.bfloat16),
            pltpu.VMEM((halo, rows, cells), jnp.float32),
            pltpu.VMEM((halo, rows, cells), jnp.float32),
            pltpu.VMEM((2, 2, rows, cells), jnp.bfloat16),
            dma((RING, GROUP)),
            dma((groups,)),
            dma((2,)),
            dma((halo,)),
            dma((halo,)),
            dma((halo,)),
            dma((halo,)),
            dma((groups,)),
            dma,
        ],
        compiler_params=pltpu.CompilerParams(
            collective_id=0, has_side_effects=True, vmem_limit_bytes=67043328
        ),
    )(table, increment, cotangent, weights)


def solution(mesh):
    placed = (
        P("lat", "lon", None, None),
        P("lat", "lon", None, None, None),
        P("lat", "lon", None, None, None, None),
        P("lat", "lon", None, None),
        P("lat", "lon", None),
    )
    return jax.shard_map(
        functools.partial(body, mesh.shape["lat"], mesh.shape["lon"]),
        mesh=mesh,
        in_specs=placed,
        out_specs=(P("lat", "lon", None, None, None), P("lat", "lon", None, None)),
        check_vma=False,
    )
```

```python
import functools

import jax
import jax.numpy as jnp
from jax import lax
from jax.experimental import pallas as pl
from jax.experimental.pallas import tpu as pltpu
from jax.sharding import PartitionSpec as P

MESH = pl.DeviceIdType.MESH
CHAINS = 4
GROUP = 8
RING = 2
PIECES = 4
SYNC = 1

PARTS = [
    [(0, 1), (0, 2)], [(3, 1), (3, 2)], [(0, 0)], [(0, 3)], [(3, 0)], [(3, 3)],
    [(1, 0), (2, 0)], [(1, 3), (2, 3)],
]
HALO = [place for part in PARTS for place in part]
FIRST = [HALO.index(part[0]) for part in PARTS]
STEP = {0: -1, 1: 0, 2: 0, 3: 1}
LEVELS = 32767.0


def kernel(
    lat_count, lon_count, targets, slots,
    inc_hbm, cot_hbm, w_hbm, ids_hbm, counts_hbm, obuf, abuf,
    wbuf, cot, ext, d0, d1, d2, d3, sendq, recvq, sends, recvs, ids, live, square, drawn, table,
    w_sem, cot_sem, own_sem, inc_send, inc_recv, adj_send, adj_recv, ids_sem, table_sem,
):
    lat = lax.axis_index("lat")
    lon = lax.axis_index("lon")
    chains = (d0, d1, d2, d3)
    groups = targets // GROUP
    quads = slots // CHAINS
    entries = targets * quads
    rows, cells = ext.shape[1], ext.shape[2]

    def load_w(g, slot, tt):
        return pltpu.make_async_copy(
            w_hbm.at[0, 0, g * GROUP + tt], wbuf.at[slot, tt], w_sem.at[slot, tt]
        )

    def load_cot(g):
        return pltpu.make_async_copy(
            cot_hbm.at[0, 0, pl.ds(g * GROUP, GROUP)], cot.at[pl.ds(g * GROUP, GROUP)], cot_sem.at[g]
        )

    wanted = [
        pltpu.make_async_copy(ids_hbm.at[0, 0], ids, ids_sem.at[0]),
        pltpu.make_async_copy(counts_hbm.at[0], live, ids_sem.at[1]),
    ]
    for copy in wanted:
        copy.start()
    own = [
        pltpu.make_async_copy(inc_hbm.at[r], ext.at[pl.ds((r + 1) * 4 + 1, 2)], own_sem.at[r])
        for r in range(2)
    ]
    for copy in own:
        copy.start()
    load_cot(0).start()
    for tt in range(GROUP):
        load_w(0, 0, tt).start()

    def exists(dlat):
        if dlat < 0:
            return lat > 0
        if dlat > 0:
            return lat < lat_count - 1
        return None

    def guarded(dlat, action):
        if dlat == 0:
            action()
        else:
            pl.when(exists(dlat))(action)

    def peer(dlat, dlon):
        return (lat + dlat, lax.rem(lon + dlon + lon_count, lon_count))

    barrier = pltpu.get_barrier_semaphore()
    around = [(a, b) for a in (-1, 0, 1) for b in (-1, 0, 1) if (a, b) != (0, 0)]
    for a, b in around:
        guarded(
            a,
            lambda a=a, b=b: pl.semaphore_signal(
                barrier, inc=1, device_id=peer(a, b), device_id_type=MESH
            ),
        )
    zero = jnp.zeros((rows, cells), jnp.float32)
    ext[16] = zero.astype(ext.dtype)
    for d in chains:
        d[entries] = zero

    def inc_copy(h):
        r, c = HALO[h]
        dlat, dlon = -STEP[r], -STEP[c]
        src = (r - 1 + 2 * (-STEP[r])) + 1, (c - 1 + 2 * (-STEP[c])) + 1
        return dlat, pltpu.make_async_remote_copy(
            src_ref=ext.at[src[0] * 4 + src[1]],
            dst_ref=ext.at[r * 4 + c],
            send_sem=inc_send.at[h],
            recv_sem=inc_recv.at[h],
            device_id=peer(dlat, dlon),
            device_id_type=MESH,
        )

    def adj_copies(d):
        r, c = PARTS[d][0]
        dlat, dlon = STEP[r], (0 if len(PARTS[d]) > 1 and r in (0, 3) else STEP[c])
        here = pl.ds(FIRST[d], len(PARTS[d]))
        return dlat, [
            pltpu.make_async_remote_copy(
                src_ref=src.at[here],
                dst_ref=dst.at[here],
                send_sem=adj_send.at[kind, d],
                recv_sem=adj_recv.at[kind, d],
                device_id=peer(dlat, dlon),
                device_id_type=MESH,
            )
            for kind, (src, dst) in enumerate(((sends, recvs), (sendq, recvq)))
        ]

    def each(copies, action):
        def run():
            for copy in copies:
                getattr(copy, action)()

        return run

    def coded(h, value):
        folded = value.reshape(rows // 8, 8, cells)
        largest = jnp.maximum(jnp.max(jnp.abs(folded), axis=0), 1e-30)
        sends[h] = largest * (1.0 / LEVELS)
        levels = jnp.round(folded * (LEVELS / largest))
        sendq[h] = levels.reshape(rows, cells).astype(jnp.int32).astype(jnp.int16)

    def decoded(h):
        levels = recvq[h].astype(jnp.int32).astype(jnp.float32)
        return (levels.reshape(rows // 8, 8, cells) * recvs[h][None]).reshape(rows, cells)

    for copy in wanted:
        copy.wait()
    draw_tables(lat, lon, lon_count, targets, slots, ids, live, square, drawn)
    to_scalars = pltpu.make_async_copy(drawn, table, table_sem)
    to_scalars.start()
    for g in range(1, groups):
        load_cot(g).start()
        if g < RING:
            for tt in range(GROUP):
                load_w(g, g, tt).start()
    to_scalars.wait()

    def adjoint_group(g, carry):
        slot = lax.rem(g, RING)
        load_cot(g).wait()
        for tt in range(GROUP):
            load_w(g, slot, tt).wait()
        for tt in range(GROUP):
            t = g * GROUP + tt
            here = cot[t]
            for q in range(quads):
                w = wbuf[slot, tt, pl.ds(q * CHAINS, CHAINS)].reshape(CHAINS * cells, cells)
                product = lax.dot_general(
                    here, w, (((1,), (1,)), ((), ())), preferred_element_type=jnp.float32
                )
                for j in range(CHAINS):
                    before = table[slots + q * CHAINS + j, t]
                    chains[j][t * quads + q] = (
                        product[:, j * cells : (j + 1) * cells] + chains[j][before]
                    )

        @pl.when(g + RING < groups)
        def _():
            for tt in range(GROUP):
                load_w(g + RING, slot, tt).start()

        return carry

    lax.fori_loop(0, SYNC, adjoint_group, 0)
    bands = exists(-1).astype(jnp.int32) + exists(1).astype(jnp.int32)
    pl.semaphore_wait(barrier, 2 + 3 * bands)

    for copy in own:
        copy.wait()
    for h in range(len(HALO)):
        dlat, copy = inc_copy(h)
        guarded(dlat, copy.start)
    lax.fori_loop(SYNC, groups, adjoint_group, 0)

    def summed(position):
        parts = [chains[j][table[2 * slots + j, position]] for j in range(CHAINS)]
        return (parts[0] + parts[1]) + (parts[2] + parts[3])

    for d, part in enumerate(PARTS):
        for h, (r, c) in enumerate(part, FIRST[d]):
            coded(h, summed(r * 4 + c))
        dlat, copies = adj_copies(d)
        guarded(dlat, each(copies, "start"))

    for h in range(len(HALO)):
        dlat, copy = inc_copy(h)
        guarded(-dlat, copy.wait_recv)
        guarded(dlat, copy.wait_send)

    def forward_group(i, carry):
        g = groups - 1 - i
        slot = lax.rem(g, RING)

        @pl.when(g < groups - RING)
        def _():
            for tt in range(GROUP):
                load_w(g, slot, tt).wait()

        for tt in range(GROUP):
            t = g * GROUP + tt
            picked = jnp.concatenate([ext[table[k, t]] for k in range(slots)], axis=1)
            w = wbuf[slot, tt].reshape(slots * cells, cells)
            obuf[0, 0, t] = jnp.dot(picked, w, preferred_element_type=jnp.float32).astype(obuf.dtype)

        @pl.when(g >= RING)
        def _():
            for tt in range(GROUP):
                load_w(g - RING, slot, tt).start()

        return carry

    lax.fori_loop(0, groups, forward_group, 0)

    index = {place: h for h, place in enumerate(HALO)}
    for dlat in (-1, 1):
        r = 0 if dlat < 0 else 3

        @pl.when(jnp.logical_not(exists(-dlat)))
        def _():
            for c in range(4):
                recvq[index[r, c]] = jnp.zeros((rows, cells), recvq.dtype)
                recvs[index[r, c]] = jnp.zeros(recvs.shape[1:], recvs.dtype)

    for d in range(len(PARTS)):
        dlat, copies = adj_copies(d)
        guarded(-dlat, each(copies, "wait_recv"))
    for a in range(2):
        for b in range(2):
            far_r, far_c = (3 if a == 0 else 0), (3 if b == 0 else 0)
            value = summed((a + 1) * 4 + b + 1)
            value += decoded(index[far_r, b + 1]) + decoded(index[a + 1, far_c])
            value += decoded(index[far_r, far_c])
            abuf[a, b] = value.astype(abuf.dtype)
    for d in range(len(PARTS)):
        dlat, copies = adj_copies(d)
        guarded(dlat, each(copies, "wait_send"))


def draw_tables(lat, lon, lon_count, targets, slots, ids, live, square, drawn):
    quads = slots // CHAINS
    cycle = 2 * lon_count
    entries = targets * quads
    number = ids[...]
    row = number // cycle - 2 * lat + 1
    col = (number % cycle - 2 * lon + 1 + cycle) % cycle
    slot = lax.broadcasted_iota(jnp.int32, (slots, targets), 0)
    position = jnp.where(slot < live[...], row * 4 + col, 16)
    drawn[pl.ds(0, slots), pl.ds(0, targets)] = position
    square[...] = jnp.full(square.shape, 16, jnp.int32)
    square[pl.ds(0, slots), pl.ds(0, targets)] = position
    turned = square[...].T
    lanes = square.shape[1]
    wide = (targets, lanes)
    behind = lax.broadcasted_iota(jnp.int32, wide, 0) * quads
    ahead = lax.broadcasted_iota(jnp.int32, wide, 1) * quads
    place = lax.broadcasted_iota(jnp.int32, wide, 1)

    def latest(found):
        best = jnp.max(functools.reduce(jnp.maximum, found), axis=0, keepdims=True)
        return jnp.where(best < 0, entries, best)

    for j in range(CHAINS):
        columns = [
            jnp.broadcast_to(turned[:targets, q * CHAINS + j : q * CHAINS + j + 1], wide) for q in range(quads)
        ]
        for q in range(quads):
            k = q * CHAINS + j
            mine = jnp.broadcast_to(square[pl.ds(k, 1), :], wide)
            found = [
                jnp.where((columns[p] == mine) & (behind + p < ahead + q), behind + p, -1)
                for p in range(quads)
            ]
            drawn[pl.ds(slots + k, 1), :] = latest(found)
        found = [jnp.where(columns[p] == place, behind + p, -1) for p in range(quads)]
        drawn[pl.ds(2 * slots + j, 1), :] = latest(found)


def write_out(ocean, adjoint, ocean_hbm, adjoint_hbm, sem):
    size = ocean.shape[2] // PIECES
    copies = [
        pltpu.make_async_copy(
            ocean.at[0, 0, pl.ds(p * size, size)], ocean_hbm.at[0, 0, pl.ds(p * size, size)], sem.at[p]
        )
        for p in range(PIECES)
    ]
    copies.append(pltpu.make_async_copy(adjoint, adjoint_hbm, sem.at[PIECES]))
    for copy in copies:
        copy.start()
    for copy in copies:
        copy.wait()


def body(lat_count, lon_count, increment, cotangent, weights, source_ids, counts):
    targets, slots = weights.shape[2], weights.shape[3]
    rows, cells = increment.shape[2], increment.shape[3]
    groups = targets // GROUP
    entries = targets * slots // CHAINS
    halo = len(HALO)
    any_space = pl.BlockSpec(memory_space=pl.ANY)
    dma = pltpu.SemaphoreType.DMA
    ocean, adjoint = pl.pallas_call(
        functools.partial(kernel, lat_count, lon_count, targets, slots),
        out_shape=(
            pltpu.VMEM(cotangent.shape, jnp.bfloat16),
            pltpu.VMEM(increment.shape, jnp.bfloat16),
        ),
        in_specs=[any_space] * 5,
        out_specs=(pl.BlockSpec(memory_space=pltpu.VMEM),) * 2,
        scratch_shapes=[
            pltpu.VMEM((RING, GROUP, slots, cells, cells), jnp.bfloat16),
            pltpu.VMEM((targets, rows, cells), jnp.bfloat16),
            pltpu.VMEM((17, rows, cells), jnp.bfloat16),
        ]
        + [pltpu.VMEM((entries + 1, rows, cells), jnp.float32)] * CHAINS
        + [
            pltpu.VMEM((halo, rows, cells), jnp.int16),
            pltpu.VMEM((halo, rows, cells), jnp.int16),
            pltpu.VMEM((halo, 8, cells), jnp.float32),
            pltpu.VMEM((halo, 8, cells), jnp.float32),
            pltpu.VMEM((slots, targets), jnp.int32),
            pltpu.VMEM((1, targets), jnp.int32),
            pltpu.VMEM((128, 128), jnp.int32),
            pltpu.VMEM((2 * slots + 8, 128), jnp.int32),
            pltpu.SMEM((2 * slots + 8, 128), jnp.int32),
            dma((RING, GROUP)),
            dma((groups,)),
            dma((2,)),
            dma((halo,)),
            dma((halo,)),
            dma((2, len(PARTS))),
            dma((2, len(PARTS))),
            dma((2,)),
            dma,
        ],
        compiler_params=pltpu.CompilerParams(
            collective_id=0, has_side_effects=True, vmem_limit_bytes=64000000
        ),
    )(increment, cotangent, weights, jnp.swapaxes(source_ids, 2, 3), counts)
    in_vmem = pl.BlockSpec(memory_space=pltpu.VMEM)
    return pl.pallas_call(
        write_out,
        out_shape=(
            jax.ShapeDtypeStruct(ocean.shape, ocean.dtype),
            jax.ShapeDtypeStruct(adjoint.shape, adjoint.dtype),
        ),
        in_specs=[in_vmem, in_vmem],
        out_specs=(any_space, any_space),
        scratch_shapes=[dma((PIECES + 1,))],
        compiler_params=pltpu.CompilerParams(vmem_limit_bytes=4 << 20),
    )(*(pltpu.with_memory_space_constraint(value, pltpu.VMEM) for value in (ocean, adjoint)))


def solution(mesh):
    placed = (
        P("lat", "lon", None, None),
        P("lat", "lon", None, None, None),
        P("lat", "lon", None, None, None, None),
        P("lat", "lon", None, None),
        P("lat", "lon", None),
    )
    return jax.shard_map(
        functools.partial(body, mesh.shape["lat"], mesh.shape["lon"]),
        mesh=mesh,
        in_specs=placed,
        out_specs=(P("lat", "lon", None, None, None), P("lat", "lon", None, None)),
        check_vma=False,
    )
```

```python
import functools

import jax
import jax.numpy as jnp
from jax import lax
from jax.experimental import pallas as pl
from jax.experimental.pallas import tpu as pltpu
from jax.sharding import PartitionSpec as P

MESH = pl.DeviceIdType.MESH
CHAINS = 4
GROUP = 8
RING = 3
PIECES = 4
SYNC = 1

PARTS = [
    [(0, 1), (0, 2)], [(3, 1), (3, 2)], [(0, 0)], [(0, 3)], [(3, 0)], [(3, 3)],
    [(1, 0), (2, 0)], [(1, 3), (2, 3)],
]
HALO = [place for part in PARTS for place in part]
FIRST = [HALO.index(part[0]) for part in PARTS]
STEP = {0: -1, 1: 0, 2: 0, 3: 1}
LEVELS = 32767.0


def kernel(
    lat_count, lon_count, targets, slots,
    inc_hbm, cot_hbm, w_hbm, ids_hbm, counts_hbm, obuf, abuf,
    wbuf, cot, ext, d0, d1, d2, d3, sendq, recvq, sends, recvs, ids, live, square, drawn, table,
    w_sem, cot_sem, own_sem, inc_send, inc_recv, adj_send, adj_recv, ids_sem, table_sem,
):
    lat = lax.axis_index("lat")
    lon = lax.axis_index("lon")
    chains = (d0, d1, d2, d3)
    groups = targets // GROUP
    quads = slots // CHAINS
    entries = targets * quads
    rows, cells = ext.shape[1], ext.shape[2]

    def load_w(g, slot, tt):
        return pltpu.make_async_copy(
            w_hbm.at[0, 0, g * GROUP + tt], wbuf.at[slot, tt], w_sem.at[slot, tt]
        )

    def load_cot(g):
        return pltpu.make_async_copy(
            cot_hbm.at[0, 0, pl.ds(g * GROUP, GROUP)], cot.at[pl.ds(g * GROUP, GROUP)], cot_sem.at[g]
        )

    wanted = [
        pltpu.make_async_copy(ids_hbm.at[0, 0], ids, ids_sem.at[0]),
        pltpu.make_async_copy(counts_hbm.at[0], live, ids_sem.at[1]),
    ]
    for copy in wanted:
        copy.start()
    own = [
        pltpu.make_async_copy(inc_hbm.at[r], ext.at[pl.ds((r + 1) * 4 + 1, 2)], own_sem.at[r])
        for r in range(2)
    ]
    for copy in own:
        copy.start()
    load_cot(0).start()
    for tt in range(GROUP):
        load_w(0, 0, tt).start()

    def exists(dlat):
        if dlat < 0:
            return lat > 0
        if dlat > 0:
            return lat < lat_count - 1
        return None

    def guarded(dlat, action):
        if dlat == 0:
            action()
        else:
            pl.when(exists(dlat))(action)

    def peer(dlat, dlon):
        return (lat + dlat, lax.rem(lon + dlon + lon_count, lon_count))

    barrier = pltpu.get_barrier_semaphore()
    around = [(a, b) for a in (-1, 0, 1) for b in (-1, 0, 1) if (a, b) != (0, 0)]
    for a, b in around:
        guarded(
            a,
            lambda a=a, b=b: pl.semaphore_signal(
                barrier, inc=1, device_id=peer(a, b), device_id_type=MESH
            ),
        )
    zero = jnp.zeros((rows, cells), jnp.float32)
    ext[16] = zero.astype(ext.dtype)
    for d in chains:
        d[entries] = zero

    def inc_copy(h):
        r, c = HALO[h]
        dlat, dlon = -STEP[r], -STEP[c]
        src = (r - 1 + 2 * (-STEP[r])) + 1, (c - 1 + 2 * (-STEP[c])) + 1
        return dlat, pltpu.make_async_remote_copy(
            src_ref=ext.at[src[0] * 4 + src[1]],
            dst_ref=ext.at[r * 4 + c],
            send_sem=inc_send.at[h],
            recv_sem=inc_recv.at[h],
            device_id=peer(dlat, dlon),
            device_id_type=MESH,
        )

    def adj_copies(d):
        r, c = PARTS[d][0]
        dlat, dlon = STEP[r], (0 if len(PARTS[d]) > 1 and r in (0, 3) else STEP[c])
        here = pl.ds(FIRST[d], len(PARTS[d]))
        return dlat, [
            pltpu.make_async_remote_copy(
                src_ref=src.at[here],
                dst_ref=dst.at[here],
                send_sem=adj_send.at[kind, d],
                recv_sem=adj_recv.at[kind, d],
                device_id=peer(dlat, dlon),
                device_id_type=MESH,
            )
            for kind, (src, dst) in enumerate(((sends, recvs), (sendq, recvq)))
        ]

    def each(copies, action):
        def run():
            for copy in copies:
                getattr(copy, action)()

        return run

    def coded(h, value):
        folded = value.reshape(rows // 8, 8, cells)
        largest = jnp.maximum(jnp.max(jnp.abs(folded), axis=0), 1e-30)
        sends[h] = largest * (1.0 / LEVELS)
        levels = jnp.round(folded * (LEVELS / largest))
        sendq[h] = levels.reshape(rows, cells).astype(jnp.int32).astype(jnp.int16)

    def decoded(h):
        levels = recvq[h].astype(jnp.int32).astype(jnp.float32)
        return (levels.reshape(rows // 8, 8, cells) * recvs[h][None]).reshape(rows, cells)

    for copy in wanted:
        copy.wait()
    draw_tables(lat, lon, lon_count, targets, slots, ids, live, square, drawn)
    to_scalars = pltpu.make_async_copy(drawn, table, table_sem)
    to_scalars.start()
    for g in range(1, groups):
        load_cot(g).start()
        if g < RING:
            for tt in range(GROUP):
                load_w(g, g, tt).start()
    to_scalars.wait()

    def adjoint_group(g, carry):
        slot = lax.rem(g, RING)
        load_cot(g).wait()
        for tt in range(GROUP):
            load_w(g, slot, tt).wait()
        for tt in range(GROUP):
            t = g * GROUP + tt
            here = cot[t]
            for q in range(quads):
                w = wbuf[slot, tt, pl.ds(q * CHAINS, CHAINS)].reshape(CHAINS * cells, cells)
                product = lax.dot_general(
                    here, w, (((1,), (1,)), ((), ())), preferred_element_type=jnp.float32
                )
                for j in range(CHAINS):
                    before = table[slots + q * CHAINS + j, t]
                    chains[j][t * quads + q] = (
                        product[:, j * cells : (j + 1) * cells] + chains[j][before]
                    )

        @pl.when(g + RING < groups)
        def _():
            for tt in range(GROUP):
                load_w(g + RING, slot, tt).start()

        return carry

    lax.fori_loop(0, SYNC, adjoint_group, 0)
    bands = exists(-1).astype(jnp.int32) + exists(1).astype(jnp.int32)
    pl.semaphore_wait(barrier, 2 + 3 * bands)

    for copy in own:
        copy.wait()
    for h in range(len(HALO)):
        dlat, copy = inc_copy(h)
        guarded(dlat, copy.start)
    lax.fori_loop(SYNC, groups, adjoint_group, 0)

    def summed(position):
        parts = [chains[j][table[2 * slots + j, position]] for j in range(CHAINS)]
        return (parts[0] + parts[1]) + (parts[2] + parts[3])

    for d, part in enumerate(PARTS):
        for h, (r, c) in enumerate(part, FIRST[d]):
            coded(h, summed(r * 4 + c))
        dlat, copies = adj_copies(d)
        guarded(dlat, each(copies, "start"))

    for h in range(len(HALO)):
        dlat, copy = inc_copy(h)
        guarded(-dlat, copy.wait_recv)
        guarded(dlat, copy.wait_send)

    def forward_group(i, carry):
        g = groups - 1 - i
        slot = lax.rem(g, RING)

        @pl.when(g < groups - RING)
        def _():
            for tt in range(GROUP):
                load_w(g, slot, tt).wait()

        for tt in range(GROUP):
            t = g * GROUP + tt
            picked = jnp.concatenate([ext[table[k, t]] for k in range(slots)], axis=1)
            w = wbuf[slot, tt].reshape(slots * cells, cells)
            obuf[0, 0, t] = jnp.dot(picked, w, preferred_element_type=jnp.float32).astype(obuf.dtype)

        @pl.when(g >= RING)
        def _():
            for tt in range(GROUP):
                load_w(g - RING, slot, tt).start()

        return carry

    lax.fori_loop(0, groups, forward_group, 0)

    index = {place: h for h, place in enumerate(HALO)}
    for dlat in (-1, 1):
        r = 0 if dlat < 0 else 3

        @pl.when(jnp.logical_not(exists(-dlat)))
        def _():
            for c in range(4):
                recvq[index[r, c]] = jnp.zeros((rows, cells), recvq.dtype)
                recvs[index[r, c]] = jnp.zeros(recvs.shape[1:], recvs.dtype)

    for d in range(len(PARTS)):
        dlat, copies = adj_copies(d)
        guarded(-dlat, each(copies, "wait_recv"))
    for a in range(2):
        for b in range(2):
            far_r, far_c = (3 if a == 0 else 0), (3 if b == 0 else 0)
            value = summed((a + 1) * 4 + b + 1)
            value += decoded(index[far_r, b + 1]) + decoded(index[a + 1, far_c])
            value += decoded(index[far_r, far_c])
            abuf[a, b] = value.astype(abuf.dtype)
    for d in range(len(PARTS)):
        dlat, copies = adj_copies(d)
        guarded(dlat, each(copies, "wait_send"))


def draw_tables(lat, lon, lon_count, targets, slots, ids, live, square, drawn):
    quads = slots // CHAINS
    cycle = 2 * lon_count
    entries = targets * quads
    number = ids[...]
    row = number // cycle - 2 * lat + 1
    col = (number % cycle - 2 * lon + 1 + cycle) % cycle
    slot = lax.broadcasted_iota(jnp.int32, (slots, targets), 0)
    position = jnp.where(slot < live[...], row * 4 + col, 16)
    drawn[pl.ds(0, slots), pl.ds(0, targets)] = position
    square[...] = jnp.full(square.shape, 16, jnp.int32)
    square[pl.ds(0, slots), pl.ds(0, targets)] = position
    turned = square[...].T
    lanes = square.shape[1]
    wide = (targets, lanes)
    behind = lax.broadcasted_iota(jnp.int32, wide, 0) * quads
    ahead = lax.broadcasted_iota(jnp.int32, wide, 1) * quads
    place = lax.broadcasted_iota(jnp.int32, wide, 1)

    def latest(found):
        best = jnp.max(functools.reduce(jnp.maximum, found), axis=0, keepdims=True)
        return jnp.where(best < 0, entries, best)

    for j in range(CHAINS):
        columns = [
            jnp.broadcast_to(turned[:targets, q * CHAINS + j : q * CHAINS + j + 1], wide) for q in range(quads)
        ]
        for q in range(quads):
            k = q * CHAINS + j
            mine = jnp.broadcast_to(square[pl.ds(k, 1), :], wide)
            found = [
                jnp.where((columns[p] == mine) & (behind + p < ahead + q), behind + p, -1)
                for p in range(quads)
            ]
            drawn[pl.ds(slots + k, 1), :] = latest(found)
        found = [jnp.where(columns[p] == place, behind + p, -1) for p in range(quads)]
        drawn[pl.ds(2 * slots + j, 1), :] = latest(found)


def write_out(ocean, adjoint, ocean_hbm, adjoint_hbm, sem):
    size = ocean.shape[2] // PIECES
    copies = [
        pltpu.make_async_copy(
            ocean.at[0, 0, pl.ds(p * size, size)], ocean_hbm.at[0, 0, pl.ds(p * size, size)], sem.at[p]
        )
        for p in range(PIECES)
    ]
    copies.append(pltpu.make_async_copy(adjoint, adjoint_hbm, sem.at[PIECES]))
    for copy in copies:
        copy.start()
    for copy in copies:
        copy.wait()


def body(lat_count, lon_count, increment, cotangent, weights, source_ids, counts):
    targets, slots = weights.shape[2], weights.shape[3]
    rows, cells = increment.shape[2], increment.shape[3]
    groups = targets // GROUP
    entries = targets * slots // CHAINS
    halo = len(HALO)
    any_space = pl.BlockSpec(memory_space=pl.ANY)
    dma = pltpu.SemaphoreType.DMA
    ocean, adjoint = pl.pallas_call(
        functools.partial(kernel, lat_count, lon_count, targets, slots),
        out_shape=(
            pltpu.VMEM(cotangent.shape, jnp.bfloat16),
            pltpu.VMEM(increment.shape, jnp.bfloat16),
        ),
        in_specs=[any_space] * 5,
        out_specs=(pl.BlockSpec(memory_space=pltpu.VMEM),) * 2,
        scratch_shapes=[
            pltpu.VMEM((RING, GROUP, slots, cells, cells), jnp.bfloat16),
            pltpu.VMEM((targets, rows, cells), jnp.bfloat16),
            pltpu.VMEM((17, rows, cells), jnp.bfloat16),
        ]
        + [pltpu.VMEM((entries + 1, rows, cells), jnp.float32)] * CHAINS
        + [
            pltpu.VMEM((halo, rows, cells), jnp.int16),
            pltpu.VMEM((halo, rows, cells), jnp.int16),
            pltpu.VMEM((halo, 8, cells), jnp.float32),
            pltpu.VMEM((halo, 8, cells), jnp.float32),
            pltpu.VMEM((slots, targets), jnp.int32),
            pltpu.VMEM((1, targets), jnp.int32),
            pltpu.VMEM((128, 128), jnp.int32),
            pltpu.VMEM((2 * slots + 8, 128), jnp.int32),
            pltpu.SMEM((2 * slots + 8, 128), jnp.int32),
            dma((RING, GROUP)),
            dma((groups,)),
            dma((2,)),
            dma((halo,)),
            dma((halo,)),
            dma((2, len(PARTS))),
            dma((2, len(PARTS))),
            dma((2,)),
            dma,
        ],
        compiler_params=pltpu.CompilerParams(
            collective_id=0, has_side_effects=True, vmem_limit_bytes=65300000
        ),
    )(increment, cotangent, weights, jnp.swapaxes(source_ids, 2, 3), counts)
    in_vmem = pl.BlockSpec(memory_space=pltpu.VMEM)
    return pl.pallas_call(
        write_out,
        out_shape=(
            jax.ShapeDtypeStruct(ocean.shape, ocean.dtype),
            jax.ShapeDtypeStruct(adjoint.shape, adjoint.dtype),
        ),
        in_specs=[in_vmem, in_vmem],
        out_specs=(any_space, any_space),
        scratch_shapes=[dma((PIECES + 1,))],
        compiler_params=pltpu.CompilerParams(vmem_limit_bytes=4 << 20),
    )(*(pltpu.with_memory_space_constraint(value, pltpu.VMEM) for value in (ocean, adjoint)))


def solution(mesh):
    placed = (
        P("lat", "lon", None, None),
        P("lat", "lon", None, None, None),
        P("lat", "lon", None, None, None, None),
        P("lat", "lon", None, None),
        P("lat", "lon", None),
    )
    return jax.shard_map(
        functools.partial(body, mesh.shape["lat"], mesh.shape["lon"]),
        mesh=mesh,
        in_specs=placed,
        out_specs=(P("lat", "lon", None, None, None), P("lat", "lon", None, None)),
        check_vma=False,
    )
```

```python
import functools

import jax
import jax.numpy as jnp
from jax import lax
from jax.experimental import pallas as pl
from jax.experimental.pallas import tpu as pltpu
from jax.sharding import PartitionSpec as P

MESH = pl.DeviceIdType.MESH
CHAINS = 4
GROUP = 8
RING = 3
PIECES = 4
SYNC = 1

PARTS = [
    [(3, 1), (3, 2)], [(3, 0)], [(3, 3)], [(0, 1), (0, 2)], [(0, 0)], [(0, 3)],
    [(1, 0), (2, 0)], [(1, 3), (2, 3)],
]
HALO = [place for part in PARTS for place in part]
FIRST = [HALO.index(part[0]) for part in PARTS]
STEP = {0: -1, 1: 0, 2: 0, 3: 1}
LEVELS = 32767.0


def kernel(
    lat_count, lon_count, targets, slots,
    inc_hbm, cot_hbm, w_hbm, ids_hbm, counts_hbm, obuf, abuf,
    wbuf, cot, ext, d0, d1, d2, d3, sendq, recvq, sends, recvs, mine, ids, live, square, drawn, table,
    w_sem, cot_sem, own_sem, inc_send, inc_recv, adj_send, adj_recv, ids_sem, table_sem,
):
    lat = lax.axis_index("lat")
    lon = lax.axis_index("lon")
    chains = (d0, d1, d2, d3)
    groups = targets // GROUP
    quads = slots // CHAINS
    entries = targets * quads
    rows, cells = ext.shape[1], ext.shape[2]

    def load_w(g, slot, tt):
        return pltpu.make_async_copy(
            w_hbm.at[0, 0, g * GROUP + tt], wbuf.at[slot, tt], w_sem.at[slot, tt]
        )

    def load_cot(g):
        return pltpu.make_async_copy(
            cot_hbm.at[0, 0, pl.ds(g * GROUP, GROUP)], cot.at[pl.ds(g * GROUP, GROUP)], cot_sem.at[g]
        )

    wanted = [
        pltpu.make_async_copy(ids_hbm.at[0, 0], ids, ids_sem.at[0]),
        pltpu.make_async_copy(counts_hbm.at[0], live, ids_sem.at[1]),
    ]
    for copy in wanted:
        copy.start()
    own = [
        pltpu.make_async_copy(inc_hbm.at[r], ext.at[pl.ds((r + 1) * 4 + 1, 2)], own_sem.at[r])
        for r in range(2)
    ]
    for copy in own:
        copy.start()
    load_cot(0).start()
    for tt in range(GROUP):
        load_w(0, 0, tt).start()

    def exists(dlat):
        if dlat < 0:
            return lat > 0
        if dlat > 0:
            return lat < lat_count - 1
        return None

    def guarded(dlat, action):
        if dlat == 0:
            action()
        else:
            pl.when(exists(dlat))(action)

    def peer(dlat, dlon):
        return (lat + dlat, lax.rem(lon + dlon + lon_count, lon_count))

    barrier = pltpu.get_barrier_semaphore()
    around = [(a, b) for a in (-1, 0, 1) for b in (-1, 0, 1) if (a, b) != (0, 0)]
    for a, b in around:
        guarded(
            a,
            lambda a=a, b=b: pl.semaphore_signal(
                barrier, inc=1, device_id=peer(a, b), device_id_type=MESH
            ),
        )
    zero = jnp.zeros((rows, cells), jnp.float32)
    ext[16] = zero.astype(ext.dtype)
    for d in chains:
        d[entries] = zero

    def inc_copy(h):
        r, c = HALO[h]
        dlat, dlon = -STEP[r], -STEP[c]
        src = (r - 1 + 2 * (-STEP[r])) + 1, (c - 1 + 2 * (-STEP[c])) + 1
        return dlat, pltpu.make_async_remote_copy(
            src_ref=ext.at[src[0] * 4 + src[1]],
            dst_ref=ext.at[r * 4 + c],
            send_sem=inc_send.at[h],
            recv_sem=inc_recv.at[h],
            device_id=peer(dlat, dlon),
            device_id_type=MESH,
        )

    def adj_copies(d):
        r, c = PARTS[d][0]
        dlat, dlon = STEP[r], (0 if len(PARTS[d]) > 1 and r in (0, 3) else STEP[c])
        here = pl.ds(FIRST[d], len(PARTS[d]))
        return dlat, [
            pltpu.make_async_remote_copy(
                src_ref=src.at[here],
                dst_ref=dst.at[here],
                send_sem=adj_send.at[kind, d],
                recv_sem=adj_recv.at[kind, d],
                device_id=peer(dlat, dlon),
                device_id_type=MESH,
            )
            for kind, (src, dst) in enumerate(((sends, recvs), (sendq, recvq)))
        ]

    def each(copies, action):
        def run():
            for copy in copies:
                getattr(copy, action)()

        return run

    def coded(h, value):
        folded = value.reshape(rows // 8, 8, cells)
        largest = jnp.maximum(jnp.max(jnp.abs(folded), axis=0), 1e-30)
        sends[h] = largest * (1.0 / LEVELS)
        levels = jnp.round(folded * (LEVELS / largest))
        sendq[h] = levels.reshape(rows, cells).astype(jnp.int32).astype(jnp.int16)

    def decoded(h):
        levels = recvq[h].astype(jnp.int32).astype(jnp.float32)
        return (levels.reshape(rows // 8, 8, cells) * recvs[h][None]).reshape(rows, cells)

    for copy in wanted:
        copy.wait()
    draw_tables(lat, lon, lon_count, targets, slots, ids, live, square, drawn)
    to_scalars = pltpu.make_async_copy(drawn, table, table_sem)
    to_scalars.start()
    for g in range(1, groups):
        load_cot(g).start()
        if g < RING:
            for tt in range(GROUP):
                load_w(g, g, tt).start()
    to_scalars.wait()

    def adjoint_group(g, carry):
        slot = lax.rem(g, RING)
        load_cot(g).wait()
        for tt in range(GROUP):
            load_w(g, slot, tt).wait()
        for tt in range(GROUP):
            t = g * GROUP + tt
            here = cot[t]
            for q in range(quads):
                w = wbuf[slot, tt, pl.ds(q * CHAINS, CHAINS)].reshape(CHAINS * cells, cells)
                product = lax.dot_general(
                    here, w, (((1,), (1,)), ((), ())), preferred_element_type=jnp.float32
                )
                for j in range(CHAINS):
                    before = table[slots + q * CHAINS + j, t]
                    chains[j][t * quads + q] = (
                        product[:, j * cells : (j + 1) * cells] + chains[j][before]
                    )

        @pl.when(g + RING < groups)
        def _():
            for tt in range(GROUP):
                load_w(g + RING, slot, tt).start()

        return carry

    lax.fori_loop(0, SYNC, adjoint_group, 0)
    bands = exists(-1).astype(jnp.int32) + exists(1).astype(jnp.int32)
    pl.semaphore_wait(barrier, 2 + 3 * bands)

    for copy in own:
        copy.wait()
    for h in range(len(HALO)):
        dlat, copy = inc_copy(h)
        guarded(dlat, copy.start)
    lax.fori_loop(SYNC, groups, adjoint_group, 0)

    def summed(position):
        parts = [chains[j][table[2 * slots + j, position]] for j in range(CHAINS)]
        return (parts[0] + parts[1]) + (parts[2] + parts[3])

    for d, part in enumerate(PARTS):
        for h, (r, c) in enumerate(part, FIRST[d]):
            coded(h, summed(r * 4 + c))
        dlat, copies = adj_copies(d)
        guarded(dlat, each(copies, "start"))

    for h in range(len(HALO)):
        dlat, copy = inc_copy(h)
        guarded(-dlat, copy.wait_recv)
        guarded(dlat, copy.wait_send)

    def forward_group(i, carry):
        g = groups - 1 - i
        slot = lax.rem(g, RING)

        @pl.when(g < groups - RING)
        def _():
            for tt in range(GROUP):
                load_w(g, slot, tt).wait()

        for tt in range(GROUP):
            t = g * GROUP + tt
            picked = jnp.concatenate([ext[table[k, t]] for k in range(slots)], axis=1)
            w = wbuf[slot, tt].reshape(slots * cells, cells)
            obuf[0, 0, t] = jnp.dot(picked, w, preferred_element_type=jnp.float32).astype(obuf.dtype)

        @pl.when(g >= RING)
        def _():
            for tt in range(GROUP):
                load_w(g - RING, slot, tt).start()

        return carry

    lax.fori_loop(0, groups, forward_group, 0)

    index = {place: h for h, place in enumerate(HALO)}
    for dlat in (-1, 1):
        r = 0 if dlat < 0 else 3

        @pl.when(jnp.logical_not(exists(-dlat)))
        def _():
            for c in range(4):
                recvq[index[r, c]] = jnp.zeros((rows, cells), recvq.dtype)
                recvs[index[r, c]] = jnp.zeros(recvs.shape[1:], recvs.dtype)

    for a in range(2):
        for b in range(2):
            mine[a, b] = summed((a + 1) * 4 + b + 1)
    for d in range(len(PARTS)):
        dlat, copies = adj_copies(d)
        guarded(-dlat, each(copies, "wait_recv"))
    for a in range(2):
        for b in range(2):
            far_r, far_c = (3 if a == 0 else 0), (3 if b == 0 else 0)
            value = mine[a, b]
            value += decoded(index[far_r, b + 1]) + decoded(index[a + 1, far_c])
            value += decoded(index[far_r, far_c])
            abuf[a, b] = value.astype(abuf.dtype)
    for d in range(len(PARTS)):
        dlat, copies = adj_copies(d)
        guarded(dlat, each(copies, "wait_send"))


def draw_tables(lat, lon, lon_count, targets, slots, ids, live, square, drawn):
    quads = slots // CHAINS
    cycle = 2 * lon_count
    entries = targets * quads
    number = ids[...]
    row = number // cycle - 2 * lat + 1
    col = (number % cycle - 2 * lon + 1 + cycle) % cycle
    slot = lax.broadcasted_iota(jnp.int32, (slots, targets), 0)
    position = jnp.where(slot < live[...], row * 4 + col, 16)
    drawn[pl.ds(0, slots), pl.ds(0, targets)] = position
    square[...] = jnp.full(square.shape, 16, jnp.int32)
    square[pl.ds(0, slots), pl.ds(0, targets)] = position
    turned = square[...].T
    lanes = square.shape[1]
    wide = (targets, lanes)
    behind = lax.broadcasted_iota(jnp.int32, wide, 0) * quads
    ahead = lax.broadcasted_iota(jnp.int32, wide, 1) * quads
    place = lax.broadcasted_iota(jnp.int32, wide, 1)

    def latest(found):
        best = jnp.max(functools.reduce(jnp.maximum, found), axis=0, keepdims=True)
        return jnp.where(best < 0, entries, best)

    for j in range(CHAINS):
        columns = [
            jnp.broadcast_to(turned[:targets, q * CHAINS + j : q * CHAINS + j + 1], wide) for q in range(quads)
        ]
        for q in range(quads):
            k = q * CHAINS + j
            mine = jnp.broadcast_to(square[pl.ds(k, 1), :], wide)
            found = [
                jnp.where((columns[p] == mine) & (behind + p < ahead + q), behind + p, -1)
                for p in range(quads)
            ]
            drawn[pl.ds(slots + k, 1), :] = latest(found)
        found = [jnp.where(columns[p] == place, behind + p, -1) for p in range(quads)]
        drawn[pl.ds(2 * slots + j, 1), :] = latest(found)


def write_out(ocean, adjoint, ocean_hbm, adjoint_hbm, sem):
    size = ocean.shape[2] // PIECES
    copies = [
        pltpu.make_async_copy(
            ocean.at[0, 0, pl.ds(p * size, size)], ocean_hbm.at[0, 0, pl.ds(p * size, size)], sem.at[p]
        )
        for p in range(PIECES)
    ]
    copies.append(pltpu.make_async_copy(adjoint, adjoint_hbm, sem.at[PIECES]))
    for copy in copies:
        copy.start()
    for copy in copies:
        copy.wait()


def body(lat_count, lon_count, increment, cotangent, weights, source_ids, counts):
    targets, slots = weights.shape[2], weights.shape[3]
    rows, cells = increment.shape[2], increment.shape[3]
    groups = targets // GROUP
    entries = targets * slots // CHAINS
    halo = len(HALO)
    any_space = pl.BlockSpec(memory_space=pl.ANY)
    dma = pltpu.SemaphoreType.DMA
    ocean, adjoint = pl.pallas_call(
        functools.partial(kernel, lat_count, lon_count, targets, slots),
        out_shape=(
            pltpu.VMEM(cotangent.shape, jnp.bfloat16),
            pltpu.VMEM(increment.shape, jnp.bfloat16),
        ),
        in_specs=[any_space] * 5,
        out_specs=(pl.BlockSpec(memory_space=pltpu.VMEM),) * 2,
        scratch_shapes=[
            pltpu.VMEM((RING, GROUP, slots, cells, cells), jnp.bfloat16),
            pltpu.VMEM((targets, rows, cells), jnp.bfloat16),
            pltpu.VMEM((17, rows, cells), jnp.bfloat16),
        ]
        + [pltpu.VMEM((entries + 1, rows, cells), jnp.float32)] * CHAINS
        + [
            pltpu.VMEM((halo, rows, cells), jnp.int16),
            pltpu.VMEM((halo, rows, cells), jnp.int16),
            pltpu.VMEM((halo, 8, cells), jnp.float32),
            pltpu.VMEM((halo, 8, cells), jnp.float32),
            pltpu.VMEM((2, 2, rows, cells), jnp.float32),
            pltpu.VMEM((slots, targets), jnp.int32),
            pltpu.VMEM((1, targets), jnp.int32),
            pltpu.VMEM((128, 128), jnp.int32),
            pltpu.VMEM((2 * slots + 8, 128), jnp.int32),
            pltpu.SMEM((2 * slots + 8, 128), jnp.int32),
            dma((RING, GROUP)),
            dma((groups,)),
            dma((2,)),
            dma((halo,)),
            dma((halo,)),
            dma((2, len(PARTS))),
            dma((2, len(PARTS))),
            dma((2,)),
            dma,
        ],
        compiler_params=pltpu.CompilerParams(
            collective_id=0, has_side_effects=True, vmem_limit_bytes=65300000
        ),
    )(increment, cotangent, weights, jnp.swapaxes(source_ids, 2, 3), counts)
    in_vmem = pl.BlockSpec(memory_space=pltpu.VMEM)
    return pl.pallas_call(
        write_out,
        out_shape=(
            jax.ShapeDtypeStruct(ocean.shape, ocean.dtype),
            jax.ShapeDtypeStruct(adjoint.shape, adjoint.dtype),
        ),
        in_specs=[in_vmem, in_vmem],
        out_specs=(any_space, any_space),
        scratch_shapes=[dma((PIECES + 1,))],
        compiler_params=pltpu.CompilerParams(vmem_limit_bytes=4 << 20),
    )(*(pltpu.with_memory_space_constraint(value, pltpu.VMEM) for value in (ocean, adjoint)))


def solution(mesh):
    placed = (
        P("lat", "lon", None, None),
        P("lat", "lon", None, None, None),
        P("lat", "lon", None, None, None, None),
        P("lat", "lon", None, None),
        P("lat", "lon", None),
    )
    return jax.shard_map(
        functools.partial(body, mesh.shape["lat"], mesh.shape["lon"]),
        mesh=mesh,
        in_specs=placed,
        out_specs=(P("lat", "lon", None, None, None), P("lat", "lon", None, None)),
        check_vma=False,
    )
```
